8 devices in a mesh: rep: 1 (over z), dp: 8 (over x, y, core).
Axes of the slice: x: 2, y: 2, z: 1, core: 2. Of those that a mesh axis runs over, the one named last changes fastest.
Arguments:
- g_w_gate: bfloat16 [8, 2, 1280, 4480], P(('rep', 'dp'))
- g_w_up: bfloat16 [8, 2, 1280, 4480], P(('rep', 'dp'))
- g_w_down: bfloat16 [8, 2, 4480, 1280], P(('rep', 'dp'))
- w_gate: bfloat16 [2, 1280, 4480], replicated
- w_up: bfloat16 [2, 1280, 4480], replicated
- w_down: bfloat16 [2, 4480, 1280], replicated
- m_w_gate: float32 [2, 1280, 4480], P(None, 'dp')
- m_w_up: float32 [2, 1280, 4480], P(None, 'dp')
- m_w_down: float32 [2, 4480, 1280], P(None, 'dp')
- v_w_gate: float32 [2, 1280, 4480], P(None, 'dp')
- v_w_up: float32 [2, 1280, 4480], P(None, 'dp')
- v_w_down: float32 [2, 4480, 1280], P(None, 'dp')
Outputs:
- output 1: bfloat16 [2, 1280, 4480], P('rep')
- output 2: bfloat16 [2, 1280, 4480], P('rep')
- output 3: bfloat16 [2, 4480, 1280], P('rep')
- output 4: float32 [2, 1280, 4480], P('rep', 'dp')
- output 5: float32 [2, 1280, 4480], P('rep', 'dp')
- output 6: float32 [2, 4480, 1280], P('rep', 'dp')
- output 7: float32 [2, 1280, 4480], P('rep', 'dp')
- output 8: float32 [2, 1280, 4480], P('rep', 'dp')
- output 9: float32 [2, 4480, 1280], P('rep', 'dp')
All inputs are finite; a program needn't handle non-finite values.
Results may differ from the reference program's by a relative error of at most 0.022.
Values are sent between devices in bfloat16 or wider.
A program may use at most 2 GiB of HBM per device.

```python
import jax
import jax.numpy as jnp
from jax import lax

DEVICES = 8
D = 1280
FF = 4480
LAYERS = 2
NAMES = ("w_gate", "w_up", "w_down")
SHAPES = {"w_gate": (LAYERS, D, FF), "w_up": (LAYERS, D, FF), "w_down": (LAYERS, FF, D)}


def setup_inputs(seed: int = 0, part: int = 0) -> dict:
    kz, *keys = jax.random.split(jax.random.key(seed), 1 + 5 * len(NAMES))
    loud = 2.0 ** jax.random.uniform(kz, (), jnp.float32, -1.0, 1.0)
    drawn = {}
    for name, key, both in zip(NAMES, keys[:3], keys[3:6], strict=True):
        own = jax.random.normal(jax.random.fold_in(key, part), (DEVICES, *SHAPES[name]), jnp.float32)
        shared = jax.random.normal(jax.random.fold_in(both, part), SHAPES[name], jnp.float32)
        drawn["g_" + name] = (loud * (0.7 * shared / DEVICES + 0.7 * own * DEVICES**-0.5)).astype(jnp.bfloat16)
    for name, key in zip(NAMES, keys[6:9], strict=True):
        drawn[name] = (jax.random.normal(key, SHAPES[name], jnp.float32) * SHAPES[name][1] ** -0.5).astype(jnp.bfloat16)
    for name, key in zip(NAMES, keys[9:12], strict=True):
        drawn["m_" + name] = loud * 0.5 * jax.random.normal(key, SHAPES[name], jnp.float32)
    for name, key in zip(NAMES, keys[12:15], strict=True):
        drawn["v_" + name] = loud * loud * jax.random.uniform(key, SHAPES[name], jnp.float32, 0.5, 1.5)
    return drawn


def adamw(w, m, v, g):
    m = 0.9 * m + 0.1 * g
    v = 0.95 * v + 0.05 * g * g
    step = m * lax.rsqrt(v + 1e-8) + 0.1 * w
    return (w - 0.02 * step).astype(jnp.bfloat16), m, v


def reference(g_w_gate, g_w_up, g_w_down, w_gate, w_up, w_down, m_w_gate, m_w_up, m_w_down, v_w_gate, v_w_up, v_w_down):
    def total(terms):
        return lax.scan(lambda so_far, term: (so_far + term.astype(jnp.float32), None), jnp.zeros(terms.shape[1:], jnp.float32), terms)[0]

    gradients = [total(terms).astype(jnp.bfloat16).astype(jnp.float32) for terms in (g_w_gate, g_w_up, g_w_down)]
    new = [
        adamw(w.astype(jnp.float32), m, v, g)
        for w, m, v, g in zip((w_gate, w_up, w_down), (m_w_gate, m_w_up, m_w_down), (v_w_gate, v_w_up, v_w_down), gradients, strict=True)
    ]
    return tuple(one[which] for which in range(3) for one in new)
```

```python
import functools

import jax
import jax.numpy as jnp
from jax import lax
from jax.experimental import pallas as pl
from jax.experimental.pallas import tpu as pltpu
from jax.sharding import PartitionSpec as P


BF, F32 = jnp.bfloat16, jnp.float32
ANY = pl.BlockSpec(memory_space=pl.ANY)
X, Y, CORE = 4, 2, 1
PARTS = 5
LANES = 640
ROWS = 16


class Weight:
    def __init__(self, rows, cols, first, gathered):
        self.block, self.part, self.cols, self.first, self.gathered = rows // 8, rows // 8 // PARTS, cols, first, gathered
        self.shape = 0 if cols == 1280 else 1


def step_kernel(weights, *refs):
    n = len(weights)
    steps = n * PARTS
    refs = list(refs)

    def take(count):
        out = refs[:count]
        del refs[:count]
        return out

    g, w, m, v = take(n), take(n), take(n), take(n)
    g_out = take(n)
    new = [take(1)[0] if k.gathered else take(2) for k in weights]
    from_core, from_x, from_y = take(2), take(2), take(2)
    in1, out1, in2, out2, in3, old_w, mv, g3, new3 = (take(2) for _ in range(9))
    core_send, core_recv, load1, send1, load2, send2, recv_x, recv_y, load3, save3, own_send, own_recv, hop_send, hop_recv, twin_send, twin_recv, twin2_send, twin2_recv = refs

    me = lax.axis_index("dp")

    def to(mask):
        return dict(device_id={"dp": me ^ mask}, device_id_type=pl.DeviceIdType.MESH)

    def which(t):
        wt = t // PARTS
        return wt, weights[wt], t % PARTS

    def rows(t, device):
        _, k, part = which(t)
        return pl.ds(pl.multiple_of(device * k.block + part * k.part, 16), k.part)

    def land(t):
        _, k, part = which(t)
        place = part if k.shape == 0 else t - PARTS * sum(1 for o in weights[: t // PARTS] if o.shape == 0)
        return k.shape, place

    def vector(k, units, body):
        down, across = k.part // ROWS, k.cols // LANES

        @pl.loop(0, units * down * across)
        def _(i):
            u = i // (down * across)
            j = i % (down * across)
            r = pl.multiple_of((j // across) * ROWS, ROWS)
            c = pl.multiple_of((j % across) * LANES, 128)
            body(u, (pl.ds(r, ROWS), pl.ds(c, LANES)))

    targets = (X ^ Y, X, Y, 0)

    def core_copy(t, q):
        wt, _, _ = which(t)
        s, place = land(t)
        return pltpu.make_async_remote_copy(
            g[wt].at[:, rows(t, me ^ CORE ^ targets[q])], from_core[s].at[place, q], core_send.at[t, q], core_recv.at[t, q], **to(CORE)
        )

    units1 = ((0, 0), (1, 0), (0, 1), (2, 1))

    def own1(t, u):
        wt, k, _ = which(t)
        q, layer = units1[u]
        return pltpu.make_async_copy(g[wt].at[layer, rows(t, me ^ targets[q])], in1[k.shape].at[t % 2, u, 0], load1.at[t % 2, u, 0])

    def twin1(t, u):
        s, place = land(t)
        q, layer = units1[u]
        return pltpu.make_async_copy(from_core[s].at[place, q, layer], in1[s].at[t % 2, u, 1], load1.at[t % 2, u, 1])

    def go1(t, u):
        s, place = land(t)
        mask, dst, sem = ((X, from_x, recv_x), (Y, from_y, recv_y))[u // 2]
        return pltpu.make_async_remote_copy(out1[s].at[t % 2, u], dst[s].at[place, u % 2], send1.at[t % 2, u], sem.at[t, u % 2], **to(mask))

    units2 = ((2, 0, from_x, recv_x, Y, from_y, recv_y), (1, 1, from_y, recv_y, X, from_x, recv_x))

    def loads2(t, u):
        wt, _, _ = which(t)
        s, place = land(t)
        q, layer, src = units2[u][:3]
        return [
            pltpu.make_async_copy(g[wt].at[layer, rows(t, me ^ targets[q])], in2[s].at[t % 2, u, 0], load2.at[t % 2, u, 0]),
            pltpu.make_async_copy(from_core[s].at[place, q, layer], in2[s].at[t % 2, u, 1], load2.at[t % 2, u, 1]),
            pltpu.make_async_copy(src[s].at[place, 0], in2[s].at[t % 2, u, 2], load2.at[t % 2, u, 2]),
        ]

    def go2(t, u):
        s, place = land(t)
        mask, dst, sem = units2[u][4:]
        return pltpu.make_async_remote_copy(out2[s].at[t % 2, u], dst[s].at[place, 2], send2.at[t % 2, u], sem.at[t, 2], **to(mask))

    def loads3(t, layer):
        wt, k, part = which(t)
        s, place = land(t)
        straight, summed = (from_x, from_y) if layer == 0 else (from_y, from_x)
        mine = pl.ds(part * k.part, k.part)
        slot = t % 2
        to_in = [g[wt].at[layer, rows(t, me)], from_core[s].at[place, 3, layer], straight[s].at[place, 1], summed[s].at[place, 2]]
        out = [pltpu.make_async_copy(r, in3[s].at[slot, layer, i], load3.at[slot, layer, i]) for i, r in enumerate(to_in)]
        out.append(pltpu.make_async_copy(w[wt].at[layer, rows(t, me)], old_w[s].at[slot, layer], load3.at[slot, layer, 4]))
        out.append(pltpu.make_async_copy(m[wt].at[layer, mine], mv[s].at[slot, layer, 0], load3.at[slot, layer, 5]))
        out.append(pltpu.make_async_copy(v[wt].at[layer, mine], mv[s].at[slot, layer, 1], load3.at[slot, layer, 6]))
        return out

    def saves3(t, layer):
        wt, k, part = which(t)
        s, slot = k.shape, t % 2
        mine = pl.ds(part * k.part, k.part)
        dst = new[wt].at[layer, rows(t, me)] if k.gathered else new[wt][layer].at[mine]
        return [
            pltpu.make_async_copy(g3[s].at[slot, layer], g_out[wt].at[layer, mine], save3.at[slot, layer, 0]),
            pltpu.make_async_copy(new3[s].at[slot, layer], dst, save3.at[slot, layer, 1]),
        ]

    masks = (X, Y, CORE)

    def own_copy(t, layer, i):
        wt, k, _ = which(t)
        return pltpu.make_async_remote_copy(
            new3[k.shape].at[t % 2, layer], new[wt].at[layer, rows(t, me)], own_send.at[t % 2, layer, i], own_recv.at[t, layer, i], **to(masks[i])
        )

    def pass_copy(t, layer, source, target, send, recv):
        wt, _, _ = which(t)
        place = new[wt].at[layer, rows(t, me ^ source)]
        return pltpu.make_async_remote_copy(place, place, send, recv, **to(target))

    def hop(t, layer):
        source, target = ((X, Y), (Y, X))[layer]
        return pass_copy(t, layer, source, target, hop_send.at[t, layer], hop_recv.at[t, layer])

    def twin(t, layer, i):
        return pass_copy(t, layer, masks[i], CORE, twin_send.at[t, layer, i], twin_recv.at[t, layer, i])

    def twin2(t, layer):
        return pass_copy(t, layer, X ^ Y, CORE, twin2_send.at[t, layer], twin2_recv.at[t, layer])

    def real(t):
        return 0 <= t < steps

    def gathered(t):
        return real(t) and which(t)[1].gathered

    for u in range(4):
        own1(0, u).start()
    barrier = pltpu.get_barrier_semaphore()
    for mask in masks:
        pl.semaphore_signal(barrier, inc=1, **to(mask))
    pl.semaphore_wait(barrier, 3)

    def start_core(t):
        for q in range(4):
            core_copy(t, q).start()

    def prepare1(t):
        for q in range(4):
            core_copy(t, q).wait_recv()
        for u in range(4):
            twin1(t, u).start()

    start_core(0)
    start_core(1)
    prepare1(0)
    for t in range(steps + 4):
        if real(t + 2):
            start_core(t + 2)
        if real(t):
            s, k = which(t)[1].shape, which(t)[1]
            slot = t % 2
            for u in range(4):
                own1(t, u).wait()
                twin1(t, u).wait()
            if t >= 2:
                for u in range(4):
                    go1(t - 2, u).wait_send()

            def sum1(u, at, s=s, slot=slot):
                out1[s][slot, u, *at] = (in1[s][slot, u, 0, *at].astype(F32) + in1[s][slot, u, 1, *at].astype(F32)).astype(BF)

            vector(k, 4, sum1)
            for u in (0, 2, 1, 3):
                go1(t, u).start()
        if real(t + 1):
            for u in range(4):
                own1(t + 1, u).start()
            prepare1(t + 1)
        a = t - 1
        if real(a):
            for u in range(2):
                first = go1(a, 2 * u)
                first.wait_recv()
                for c in loads2(a, u):
                    c.start()
        b = t - 2
        if real(b):
            for layer in range(2):
                (go1(b, 1) if layer == 0 else go1(b, 3)).wait_recv()
                go2(b, layer).wait_recv()
                for c in loads3(b, layer):
                    c.start()
        if real(a):
            s, k, slot = which(a)[1].shape, which(a)[1], a % 2
            for u in range(2):
                for c in loads2(a, u):
                    c.wait()
                if a >= 2:
                    go2(a - 2, u).wait_send()

            def sum2(u, at, s=s, slot=slot):
                out2[s][slot, u, *at] = (
                    in2[s][slot, u, 0, *at].astype(F32) + in2[s][slot, u, 1, *at].astype(F32) + in2[s][slot, u, 2, *at].astype(F32)
                ).astype(BF)

            vector(k, 2, sum2)
            for u in range(2):
                go2(a, u).start()
        if real(b):
            s, k, slot = which(b)[1].shape, which(b)[1], b % 2
            for layer in range(2):
                for c in loads3(b, layer):
                    c.wait()
                if b >= 2:
                    for c in saves3(b - 2, layer):
                        c.wait()
                    if gathered(b - 2):
                        for i in range(3):
                            own_copy(b - 2, layer, i).wait_send()

            def update(u, at, s=s, slot=slot):
                parts = [in3[s][slot, u, i, *at].astype(F32) for i in range(4)]
                total = (((parts[0] + parts[1]) + parts[2]) + parts[3]).astype(BF)
                g3[s][slot, u, *at] = total
                total = total.astype(F32)
                new_m = 0.9 * mv[s][slot, u, 0, *at] + 0.1 * total
                new_v = 0.95 * mv[s][slot, u, 1, *at] + 0.05 * total * total
                weight = old_w[s][slot, u, *at].astype(F32)
                new3[s][slot, u, *at] = (weight - 0.02 * (new_m * lax.rsqrt(new_v + 1e-8) + 0.1 * weight)).astype(BF)

            vector(k, 2, update)
            for layer in range(2):
                for c in saves3(b, layer):
                    c.start()
            if gathered(b):
                for layer, i in ((0, 0), (1, 1), (1, 0), (0, 1), (0, 2), (1, 2)):
                    own_copy(b, layer, i).start()
        c3 = t - 3
        if gathered(c3):
            for layer in range(2):
                own_copy(c3, layer, layer).wait_recv()
                hop(c3, layer).start()
                twin(c3, layer, layer).start()
            for layer in range(2):
                own_copy(c3, layer, 1 - layer).wait_recv()
                twin(c3, layer, 1 - layer).start()
        c4 = t - 4
        if gathered(c4):
            for layer in range(2):
                hop(c4, layer).wait_recv()
                twin2(c4, layer).start()

    for t in range(steps):
        for q in range(4):
            core_copy(t, q).wait_send()
    for t in range(steps - 2, steps):
        for u in range(4):
            go1(t, u).wait_send()
        for u in range(2):
            go2(t, u).wait_send()
            for c in saves3(t, u):
                c.wait()
            if gathered(t):
                for i in range(3):
                    own_copy(t, u, i).wait_send()
    for t in range(steps):
        if gathered(t):
            for layer in range(2):
                own_copy(t, layer, 2).wait_recv()
                hop(t, layer).wait_send()
                for i in range(2):
                    twin(t, layer, i).wait()
                twin2(t, layer).wait()


def reduce_and_step(g, w, m, v, gathered):
    weights, first = [], 0
    for one, whole in zip(w, gathered, strict=True):
        weights.append(Weight(one.shape[1], one.shape[2], first, whole))
        first += PARTS
    n, steps = len(w), first
    dims = {k.shape: (k.part, k.cols) for k in weights}
    held = {s: PARTS * sum(1 for k in weights if k.shape == s) for s in dims}
    pair = [dims[s] for s in (0, 1)]

    def hbm(*lead):
        return [jax.ShapeDtypeStruct((held[s], *lead, *dims[s]), BF) for s in (0, 1)]

    def vmem(*lead, dtype=BF):
        return [pltpu.VMEM((*lead, *d), dtype) for d in pair]

    blocks = [jax.ShapeDtypeStruct((2, k.block, k.cols), BF) for k in weights]
    out_shape = list(blocks)
    for k in weights:
        one = [jax.ShapeDtypeStruct((2, 8 * k.block, k.cols), BF)] if k.gathered else [jax.ShapeDtypeStruct((k.block, k.cols), BF)] * 2
        out_shape += one
    out_shape += hbm(4, 2) + hbm(3) + hbm(3)
    dma = pltpu.SemaphoreType.DMA
    outs = pl.pallas_call(
        functools.partial(step_kernel, weights),
        out_shape=out_shape,
        in_specs=[ANY] * (4 * n),
        out_specs=[ANY] * len(out_shape),
        scratch_shapes=[
            *vmem(2, 4, 2),
            *vmem(2, 4),
            *vmem(2, 2, 3),
            *vmem(2, 2),
            *vmem(2, 2, 4),
            *vmem(2, 2),
            *vmem(2, 2, 2, dtype=F32),
            *vmem(2, 2),
            *vmem(2, 2),
            dma((steps, 4)),
            dma((steps, 4)),
            dma((2, 4, 2)),
            dma((2, 4)),
            dma((2, 2, 3)),
            dma((2, 2)),
            dma((steps, 3)),
            dma((steps, 3)),
            dma((2, 2, 7)),
            dma((2, 2, 2)),
            dma((2, 2, 3)),
            dma((steps, 2, 3)),
            dma((steps, 2)),
            dma((steps, 2)),
            dma((steps, 2, 2)),
            dma((steps, 2, 2)),
            dma((steps, 2)),
            dma((steps, 2)),
        ],
        compiler_params=pltpu.CompilerParams(collective_id=0, has_side_effects=True, vmem_limit_bytes=60 << 20),
        cost_estimate=pl.CostEstimate(flops=10**9, bytes_accessed=4 * 10**8, transcendentals=10**7),
        name="reduce_and_step",
    )(*g, *w, *m, *v)
    rest = list(outs[n:])
    return outs[:n], [rest.pop(0) if k.gathered else (rest.pop(0), rest.pop(0)) for k in weights]


def cost(bytes_accessed, flops):
    return pl.CostEstimate(flops=flops, bytes_accessed=bytes_accessed, transcendentals=0)


def copied(x):
    layers, rows, cols = x.shape
    part, slots = rows // 8, 8
    pieces = [(layer, i) for layer in range(layers) for i in range(8)]

    def body(src, dst, held, sem_in, sem_out):
        def get(j):
            layer, i = pieces[j]
            return pltpu.make_async_copy(src.at[layer, pl.ds(i * part, part)], held.at[j % slots], sem_in.at[j % slots])

        def put(j):
            layer, i = pieces[j]
            return pltpu.make_async_copy(held.at[j % slots], dst.at[layer, pl.ds(i * part, part)], sem_out.at[j % slots])

        lag = slots // 2
        for j in range(len(pieces) + lag):
            if j < len(pieces):
                if j >= slots:
                    put(j - slots).wait()
                get(j).start()
            if j >= lag:
                get(j - lag).wait()
                put(j - lag).start()
        for j in range(len(pieces) - slots, len(pieces)):
            put(j).wait()

    return pl.pallas_call(
        body,
        out_shape=jax.ShapeDtypeStruct(x.shape, x.dtype),
        in_specs=[ANY],
        out_specs=ANY,
        scratch_shapes=[pltpu.VMEM((slots, part, cols), x.dtype), pltpu.SemaphoreType.DMA((slots,)), pltpu.SemaphoreType.DMA((slots,))],
        cost_estimate=cost(4 * x.size, 10**8),
        name="copied",
    )(x)


def placed(pieces, out, rows):
    n, cols = len(pieces), pieces[0][0].shape[-1]

    def body(*refs):
        src, (dst, held, sem) = refs[:n], refs[-3:]
        me = lax.axis_index("dp")
        gets = [pltpu.make_async_copy(src[i], held.at[i], sem.at[0, i]) for i in range(n)]
        puts = []
        for i, (_, layer, mask) in enumerate(pieces):
            to = pl.ds(pl.multiple_of((me ^ mask) * rows, 16), rows)
            puts.append(pltpu.make_async_copy(held.at[i], dst.at[layer, to], sem.at[1, i]))
        for c in gets:
            c.start()
        for a, b in zip(gets, puts, strict=True):
            a.wait()
            b.start()
        for c in puts:
            c.wait()

    args = [one[0] for one in pieces] + ([] if out is None else [out])
    return pl.pallas_call(
        body,
        out_shape=jax.ShapeDtypeStruct((2, rows * 8, cols), BF),
        in_specs=[ANY] * len(args),
        out_specs=ANY,
        input_output_aliases={} if out is None else {n: 0},
        scratch_shapes=[pltpu.VMEM((n, rows, cols), BF), pltpu.SemaphoreType.DMA((2, n))],
        cost_estimate=cost(4 * n * rows * cols, 10**7),
        name="placed",
    )(*args)


def moved(x, mask):
    return lax.ppermute(x, "dp", [(i, i ^ mask) for i in range(8)])


def moments(m, v, g):
    g = g.astype(F32)
    return 0.9 * m + 0.1 * g, 0.95 * v + 0.05 * g * g


def solution(mesh):
    def inner(*arrays):
        terms, weights, m, v = (arrays[i : i + 3] for i in (0, 3, 6, 9))
        order = (2, 0, 1)
        sums, new = reduce_and_step([terms[i][0] for i in order], [weights[i] for i in order], [m[i] for i in order], [v[i] for i in order], (False, True, True))
        sums = [sums[order.index(i)] for i in range(3)]
        (A, B), gate, up = new
        rows = A.shape[0]
        xA, yB, xB, yA = moved(A, X), moved(B, Y), moved(B, X), moved(A, Y)
        cA, cB = moved(A, CORE), moved(B, CORE)
        dA, dB = moved(xA, Y), moved(yB, X)
        gate = copied(gate)
        up = copied(up)
        down = placed([(A, 0, 0), (B, 1, 0), (cA, 0, CORE), (cB, 1, CORE)], None, rows)
        cxA, cyB, cxB, cyA = moved(xA, CORE), moved(yB, CORE), moved(xB, CORE), moved(yA, CORE)
        down = placed([(xA, 0, X), (xB, 1, X), (yA, 0, Y), (yB, 1, Y)], down, rows)
        down = placed([(cxA, 0, X + CORE), (cxB, 1, X + CORE), (cyA, 0, Y + CORE), (cyB, 1, Y + CORE)], down, rows)
        cdA, cdB = moved(dA, CORE), moved(dB, CORE)
        down = placed([(dA, 0, X + Y), (dB, 1, X + Y)], down, rows)
        down = placed([(cdA, 0, X + Y + CORE), (cdB, 1, X + Y + CORE)], down, rows)
        after = []
        for i in range(3):
            after.append(moments(m[i], v[i], sums[i]))
        return (gate, up, down, *(one[0] for one in after), *(one[1] for one in after))

    all_of, cut = P(None, None, None), P(None, "dp", None)
    return jax.shard_map(
        inner,
        mesh=mesh,
        in_specs=(P(("rep", "dp"), None, None, None),) * 3 + (all_of,) * 3 + (cut,) * 6,
        out_specs=(P("rep", None, None),) * 3 + (P("rep", "dp", None),) * 6,
        check_vma=False,
    )
```

```python
import functools

import jax
import jax.numpy as jnp
from jax import lax
from jax.experimental import pallas as pl
from jax.experimental.pallas import tpu as pltpu
from jax.sharding import PartitionSpec as P


BF, F32 = jnp.bfloat16, jnp.float32
ANY = pl.BlockSpec(memory_space=pl.ANY)
X, Y, CORE = 4, 2, 1
LANES = 640
ROWS = 16


class Weight:
    def __init__(self, w, cuts, split=None):
        self.block, self.cols, self.cuts, self.split = w.shape[1] // 8, w.shape[2], cuts, split
        self.gathered = split is None
        self.shape = 0 if self.cols == 1280 else 1
        assert sum(cuts) == self.block and (split is None or split in [sum(cuts[:i]) for i in range(len(cuts))])


def step_kernel(weights, *refs):
    n = len(weights)
    plan = [(i, sum(k.cuts[:j]), rows) for i, k in enumerate(weights) for j, rows in enumerate(k.cuts)]
    steps = len(plan)
    refs = list(refs)

    def take(count):
        out = refs[:count]
        del refs[:count]
        return out

    g, w, m, v = take(n), take(n), take(n), take(n)
    g_out = take(n)
    new = [take(1)[0] if k.gathered else take(8) for k in weights]
    from_core, from_x, from_y = take(n), take(n), take(n)
    in1, out1, in2, out2, in3, old_w, mv, g3, new3 = (take(2) for _ in range(9))
    core_send, core_recv, load1, send1, load2, send2, recv_x, recv_y, load3, save3, own_send, own_recv, hop_send, hop_recv, twin_send, twin_recv, twin2_send, twin2_recv = refs

    me = lax.axis_index("dp")

    def to(mask):
        return dict(device_id={"dp": me ^ mask}, device_id_type=pl.DeviceIdType.MESH)

    def which(t):
        wt, first, size = plan[t]
        return wt, weights[wt].shape, first, size

    def rows(t, device):
        wt, _, first, size = which(t)
        return pl.ds(pl.multiple_of(device * weights[wt].block + first, 16), size)

    def mine(t):
        return pl.ds(plan[t][1], plan[t][2])

    def held(t, ref, *at):
        ref = ref[which(t)[1]]
        return ref.at[(t % ref.shape[0], *at, pl.ds(0, plan[t][2]))]

    def vector(t, units, body):
        wt, s, _, size = which(t)
        down, across = size // ROWS, weights[wt].cols // LANES

        @pl.loop(0, units * down * across)
        def _(i):
            u = i // (down * across)
            j = i % (down * across)
            r = pl.multiple_of((j // across) * ROWS, ROWS)
            c = pl.multiple_of((j % across) * LANES, 128)
            body(s, t % 2, u, (pl.ds(r, ROWS), pl.ds(c, LANES)))

    targets = (X ^ Y, X, Y, 0)

    def core_copy(t, q):
        wt = plan[t][0]
        return pltpu.make_async_remote_copy(
            g[wt].at[:, rows(t, me ^ CORE ^ targets[q])], from_core[wt].at[q, :, mine(t)], core_send.at[t, q], core_recv.at[t, q], **to(CORE)
        )

    units1 = ((0, 0), (1, 0), (0, 1), (2, 1))

    def own1(t, u):
        q, layer = units1[u]
        return pltpu.make_async_copy(g[plan[t][0]].at[layer, rows(t, me ^ targets[q])], held(t, in1, u, 0), load1.at[t % 2, u, 0])

    def twin1(t, u):
        q, layer = units1[u]
        return pltpu.make_async_copy(from_core[plan[t][0]].at[q, layer, mine(t)], held(t, in1, u, 1), load1.at[t % 2, u, 1])

    def go1(t, u):
        mask, dst, sem = ((X, from_x, recv_x), (Y, from_y, recv_y))[u // 2]
        return pltpu.make_async_remote_copy(held(t, out1, u), dst[plan[t][0]].at[u % 2, mine(t)], send1.at[t % 2, u], sem.at[t, u % 2], **to(mask))

    units2 = ((2, 0, from_x, Y, from_y, recv_y), (1, 1, from_y, X, from_x, recv_x))

    def loads2(t, u):
        wt = plan[t][0]
        q, layer, src = units2[u][:3]
        sources = (g[wt].at[layer, rows(t, me ^ targets[q])], from_core[wt].at[q, layer, mine(t)], src[wt].at[0, mine(t)])
        return [pltpu.make_async_copy(r, held(t, in2, u, i), load2.at[t % 2, u, i]) for i, r in enumerate(sources)]

    def go2(t, u):
        mask, dst, sem = units2[u][3:]
        return pltpu.make_async_remote_copy(held(t, out2, u), dst[plan[t][0]].at[2, mine(t)], send2.at[t % 2, u], sem.at[t, 2], **to(mask))

    def loads3(t, layer):
        wt = plan[t][0]
        straight, summed = (from_x, from_y) if layer == 0 else (from_y, from_x)
        moves = [
            (g[wt].at[layer, rows(t, me)], held(t, in3, layer, 0)),
            (from_core[wt].at[3, layer, mine(t)], held(t, in3, layer, 1)),
            (w[wt].at[layer, rows(t, me)], held(t, old_w, layer)),
            (m[wt].at[layer, mine(t)], held(t, mv, layer, 0)),
            (v[wt].at[layer, mine(t)], held(t, mv, layer, 1)),
            (straight[wt].at[1, mine(t)], held(t, in3, layer, 2)),
            (summed[wt].at[2, mine(t)], held(t, in3, layer, 3)),
        ]
        return [pltpu.make_async_copy(a, b, load3.at[t % 2, layer, i]) for i, (a, b) in enumerate(moves)]

    def piece(t, layer):
        wt, _, first, _ = which(t)
        k = weights[wt]
        return (new[wt][2 + 2 * layer], first) if first < k.split else (new[wt][3 + 2 * layer], first - k.split)

    def saves3(t, layer):
        wt, _, _, size = which(t)
        places = [g_out[wt].at[layer, mine(t)]]
        if weights[wt].gathered:
            places.append(new[wt].at[layer, rows(t, me)])
        else:
            ref, at = piece(t, layer)
            places += [new[wt][layer].at[mine(t)], ref.at[pl.ds(at, size)]]
        return [
            pltpu.make_async_copy(held(t, g3 if i == 0 else new3, layer), place, save3.at[t % 2, layer, i]) for i, place in enumerate(places)
        ]

    masks = (X, Y, CORE)

    def own_copy(t, layer, i):
        wt = plan[t][0]
        dst = new[wt].at[layer, rows(t, me)] if weights[wt].gathered else new[wt][6 + layer].at[mine(t)]
        return pltpu.make_async_remote_copy(held(t, new3, layer), dst, own_send.at[t % 2, layer, i], own_recv.at[t, layer, i], **to(masks[i]))

    def neighbours(t):
        return range(3) if gathered(t) else (2,)

    def pass_copy(t, layer, source, target, send, recv):
        place = new[plan[t][0]].at[layer, rows(t, me ^ source)]
        return pltpu.make_async_remote_copy(place, place, send, recv, **to(target))

    def hop(t, layer):
        source, target = ((X, Y), (Y, X))[layer]
        return pass_copy(t, layer, source, target, hop_send.at[t, layer], hop_recv.at[t, layer])

    def twin(t, layer, i):
        return pass_copy(t, layer, masks[i], CORE, twin_send.at[t, layer, i], twin_recv.at[t, layer, i])

    def twin2(t, layer):
        return pass_copy(t, layer, X ^ Y, CORE, twin2_send.at[t, layer], twin2_recv.at[t, layer])

    def real(t):
        return 0 <= t < steps

    def gathered(t):
        return real(t) and weights[plan[t][0]].gathered

    for u in range(4):
        own1(0, u).start()
    barrier = pltpu.get_barrier_semaphore()
    for mask in masks:
        pl.semaphore_signal(barrier, inc=1, **to(mask))
    pl.semaphore_wait(barrier, 3)

    def start_core(t):
        for q in range(4):
            core_copy(t, q).start()

    def prepare1(t):
        for q in range(4):
            core_copy(t, q).wait_recv()
        for u in range(4):
            twin1(t, u).start()

    start_core(0)
    start_core(1)
    prepare1(0)
    for t in range(steps + 4):
        if real(t + 2):
            start_core(t + 2)
        if real(t):
            for u in range(4):
                own1(t, u).wait()
                twin1(t, u).wait()
            if t >= 2:
                for u in range(4):
                    go1(t - 2, u).wait_send()

            def sum1(s, slot, u, at):
                out1[s][slot, u, *at] = (in1[s][0, u, 0, *at].astype(F32) + in1[s][0, u, 1, *at].astype(F32)).astype(BF)

            vector(t, 4, sum1)
            for u in (0, 2, 1, 3):
                go1(t, u).start()
        if real(t + 1):
            for u in range(4):
                own1(t + 1, u).start()
            prepare1(t + 1)
        a = t - 1
        if real(a):
            for u in range(2):
                for c in loads2(a, u)[:2]:
                    c.start()
            for u in range(2):
                go1(a, 2 * u).wait_recv()
                loads2(a, u)[2].start()
            for u in range(2):
                for c in loads2(a, u):
                    c.wait()
                if a >= 2:
                    go2(a - 2, u).wait_send()

            def sum2(s, slot, u, at):
                out2[s][slot, u, *at] = (
                    in2[s][0, u, 0, *at].astype(F32) + in2[s][0, u, 1, *at].astype(F32) + in2[s][0, u, 2, *at].astype(F32)
                ).astype(BF)

            vector(a, 2, sum2)
            for u in range(2):
                go2(a, u).start()
        b = t - 2
        if real(b):
            for layer in range(2):
                for c in loads3(b, layer)[:5]:
                    c.start()
            for layer in range(2):
                go1(b, 1 + 2 * layer).wait_recv()
                go2(b, layer).wait_recv()
                for c in loads3(b, layer)[5:]:
                    c.start()
            for layer in range(2):
                for c in loads3(b, layer):
                    c.wait()
                if b >= 2:
                    for c in saves3(b - 2, layer):
                        c.wait()
                    for i in neighbours(b - 2):
                        own_copy(b - 2, layer, i).wait_send()

            def update(s, slot, u, at):
                parts = [in3[s][0, u, i, *at].astype(F32) for i in range(4)]
                total = (((parts[0] + parts[1]) + parts[2]) + parts[3]).astype(BF)
                g3[s][slot, u, *at] = total
                total = total.astype(F32)
                new_m = 0.9 * mv[s][0, u, 0, *at] + 0.1 * total
                new_v = 0.95 * mv[s][0, u, 1, *at] + 0.05 * total * total
                weight = old_w[s][0, u, *at].astype(F32)
                new3[s][slot, u, *at] = (weight - 0.02 * (new_m * lax.rsqrt(new_v + 1e-8) + 0.1 * weight)).astype(BF)

            vector(b, 2, update)
            if gathered(b):
                for layer, i in ((0, 0), (1, 1), (1, 0), (0, 1)):
                    own_copy(b, layer, i).start()
            for layer in range(2):
                own_copy(b, layer, 2).start()
                for c in saves3(b, layer):
                    c.start()
        c3 = t - 3
        if gathered(c3):
            for layer in range(2):
                own_copy(c3, layer, layer).wait_recv()
                hop(c3, layer).start()
                twin(c3, layer, layer).start()
            for layer in range(2):
                own_copy(c3, layer, 1 - layer).wait_recv()
                twin(c3, layer, 1 - layer).start()
        c4 = t - 4
        if gathered(c4):
            for layer in range(2):
                hop(c4, layer).wait_recv()
                twin2(c4, layer).start()

    for t in range(steps):
        for q in range(4):
            core_copy(t, q).wait_send()
    for t in range(steps - 2, steps):
        for u in range(4):
            go1(t, u).wait_send()
        for u in range(2):
            go2(t, u).wait_send()
            for c in saves3(t, u):
                c.wait()
            for i in neighbours(t):
                own_copy(t, u, i).wait_send()
    for t in range(steps):
        for layer in range(2):
            own_copy(t, layer, 2).wait_recv()
            if gathered(t):
                hop(t, layer).wait_send()
                for i in range(2):
                    twin(t, layer, i).wait()
                twin2(t, layer).wait()


def reduce_and_step(g, w, m, v, cuts, split):
    weights = [Weight(one, cut, split if i == 0 else None) for i, (one, cut) in enumerate(zip(w, cuts, strict=True))]
    n, steps = len(w), sum(len(cut) for cut in cuts)
    pair = [max((max(k.cuts), k.cols) for k in weights if k.shape == s) for s in (0, 1)]

    def hbm(*lead):
        return [jax.ShapeDtypeStruct((*lead, k.block, k.cols), BF) for k in weights]

    def vmem(*lead, dtype=BF):
        return [pltpu.VMEM((*lead, *d), dtype) for d in pair]

    out_shape = hbm(2)
    for k in weights:
        sizes = (k.block, k.block, k.split, k.block - k.split, k.split, k.block - k.split, k.block, k.block) if k.split else ()
        out_shape += [jax.ShapeDtypeStruct((size, k.cols), BF) for size in sizes] or [jax.ShapeDtypeStruct((2, 8 * k.block, k.cols), BF)]
    out_shape += hbm(4, 2) + hbm(3) + hbm(3)
    dma = pltpu.SemaphoreType.DMA
    outs = pl.pallas_call(
        functools.partial(step_kernel, weights),
        out_shape=out_shape,
        in_specs=[ANY] * (4 * n),
        out_specs=[ANY] * len(out_shape),
        scratch_shapes=[
            *vmem(1, 4, 2),
            *vmem(2, 4),
            *vmem(1, 2, 3),
            *vmem(2, 2),
            *vmem(1, 2, 4),
            *vmem(1, 2),
            *vmem(1, 2, 2, dtype=F32),
            *vmem(2, 2),
            *vmem(2, 2),
            dma((steps, 4)),
            dma((steps, 4)),
            dma((2, 4, 2)),
            dma((2, 4)),
            dma((2, 2, 3)),
            dma((2, 2)),
            dma((steps, 3)),
            dma((steps, 3)),
            dma((2, 2, 7)),
            dma((2, 2, 3)),
            dma((2, 2, 3)),
            dma((steps, 2, 3)),
            dma((steps, 2)),
            dma((steps, 2)),
            dma((steps, 2, 2)),
            dma((steps, 2, 2)),
            dma((steps, 2)),
            dma((steps, 2)),
        ],
        compiler_params=pltpu.CompilerParams(collective_id=0, has_side_effects=True, vmem_limit_bytes=60 << 20),
        cost_estimate=pl.CostEstimate(flops=10**9, bytes_accessed=4 * 10**8, transcendentals=10**7),
        name="reduce_and_step",
    )(*g, *w, *m, *v)
    return outs[:n], outs[n : n + 8], outs[n + 8 : 2 * n + 7]


def cost(bytes_accessed, flops):
    return pl.CostEstimate(flops=flops, bytes_accessed=bytes_accessed, transcendentals=0)


def copied(x):
    layers, rows, cols = x.shape
    part, slots = rows // 8, 8
    pieces = [(layer, i) for layer in range(layers) for i in range(8)]

    def body(src, dst, held, sem_in, sem_out):
        def get(j):
            layer, i = pieces[j]
            return pltpu.make_async_copy(src.at[layer, pl.ds(i * part, part)], held.at[j % slots], sem_in.at[j % slots])

        def put(j):
            layer, i = pieces[j]
            return pltpu.make_async_copy(held.at[j % slots], dst.at[layer, pl.ds(i * part, part)], sem_out.at[j % slots])

        lag = slots // 2
        for j in range(len(pieces) + lag):
            if j < len(pieces):
                if j >= slots:
                    put(j - slots).wait()
                get(j).start()
            if j >= lag:
                get(j - lag).wait()
                put(j - lag).start()
        for j in range(len(pieces) - slots, len(pieces)):
            put(j).wait()

    return pl.pallas_call(
        body,
        out_shape=jax.ShapeDtypeStruct(x.shape, x.dtype),
        in_specs=[ANY],
        out_specs=ANY,
        scratch_shapes=[pltpu.VMEM((slots, part, cols), x.dtype), pltpu.SemaphoreType.DMA((slots,)), pltpu.SemaphoreType.DMA((slots,))],
        cost_estimate=cost(4 * x.size, 10**8),
        compiler_params=pltpu.CompilerParams(vmem_limit_bytes=16 << 20),
        name="copied",
    )(x)


def placed(pieces, out, block, near=True):
    n, cols = len(pieces), pieces[0][0].shape[-1]

    def body(*refs):
        src, (dst, *held, sem) = refs[:n], refs[n if out is None else n + 1 :]
        me = lax.axis_index("dp")
        if not near:
            gets = [pltpu.make_async_copy(a, b, sem.at[n + i]) for i, (a, b) in enumerate(zip(src, held, strict=True))]
            for c in gets:
                c.start()
            src = held
        puts = []
        for i, (one, layer, mask, first) in enumerate(pieces):
            to = pl.ds(pl.multiple_of((me ^ mask) * block + first, 16), one.shape[0])
            puts.append(pltpu.make_async_copy(src[i], dst.at[layer, to], sem.at[i]))
            if not near:
                gets[i].wait()
            puts[i].start()
        for c in puts:
            c.wait()

    args = [one[0] for one in pieces] + ([] if out is None else [out])
    scratch = [] if near else [pltpu.VMEM(one[0].shape, BF) for one in pieces]
    return pl.pallas_call(
        body,
        out_shape=jax.ShapeDtypeStruct((2, block * 8, cols), BF),
        in_specs=[pl.BlockSpec(memory_space=pltpu.VMEM) if near else ANY] * n + [ANY] * (len(args) - n),
        out_specs=ANY,
        input_output_aliases={} if out is None else {n: 0},
        scratch_shapes=[*scratch, pltpu.SemaphoreType.DMA((2 * n,))],
        cost_estimate=cost(4 * sum(one[0].size for one in pieces), 10**7),
        compiler_params=pltpu.CompilerParams(vmem_limit_bytes=8 << 20),
        name="placed",
    )(*args)


def moved(x, mask):
    return lax.ppermute(x, "dp", [(i, i ^ mask) for i in range(8)])


def moments(m, v, g):
    g = g.astype(F32)
    return 0.9 * m + 0.1 * g, 0.95 * v + 0.05 * g * g


CUTS = ((16, 48, 96, 128, 144, 128), (80, 80), (64, 48, 32, 16))
SPLIT = 432


def solution(mesh):
    def inner(*arrays):
        terms, weights, m, v = (arrays[i : i + 3] for i in (0, 3, 6, 9))
        order = (2, 0, 1)
        sums, mine, (gate, up) = reduce_and_step(
            [terms[i][0] for i in order], [weights[i] for i in order], [m[i] for i in order], [v[i] for i in order], CUTS, SPLIT
        )
        sums = [sums[order.index(i)] for i in range(3)]
        A, B, A0, A1, B0, B1, cA, cB = mine
        rows = A.shape[0]
        xA0, yB0, xA1, yB1 = moved(A0, X), moved(B0, Y), moved(A1, X), moved(B1, Y)
        xB, yA = moved(B, X), moved(A, Y)
        dA0, dB0, dA1, dB1 = moved(xA0, Y), moved(yB0, X), moved(xA1, Y), moved(yB1, X)
        gate = copied(gate)
        up = copied(up)

        def place(i, down, *pieces):
            return placed(pieces, down, rows, near=i > 0)

        def twins(*pieces):
            return [(moved(x, CORE), layer, mask + CORE, first) for x, layer, mask, first in pieces]

        near = [(xA0, 0, X, 0), (yB0, 1, Y, 0), (xA1, 0, X, SPLIT), (yB1, 1, Y, SPLIT), (xB, 1, X, 0), (yA, 0, Y, 0)]
        far0, far1 = [(dA0, 0, X + Y, 0), (dB0, 1, X + Y, 0)], [(dA1, 0, X + Y, SPLIT), (dB1, 1, X + Y, SPLIT)]
        down = place(0, None, (A, 0, 0, 0), (B, 1, 0, 0), (cA, 0, CORE, 0), (cB, 1, CORE, 0))
        down = place(1, down, *near)
        down = place(2, down, *twins(*near))
        down = place(3, down, *far0)
        down = place(4, down, *twins(*far0))
        down = place(5, down, *far1)
        last = [(moved(x, CORE), layer, mask + CORE, first) for x, layer, mask, first in far1]
        down = place(6, down, *last)
        after = []
        for i in range(3):
            after.append(moments(m[i], v[i], sums[i]))
        return (gate, up, down, *(one[0] for one in after), *(one[1] for one in after))

    all_of, cut = P(None, None, None), P(None, "dp", None)
    return jax.shard_map(
        inner,
        mesh=mesh,
        in_specs=(P(("rep", "dp"), None, None, None),) * 3 + (all_of,) * 3 + (cut,) * 6,
        out_specs=(P("rep", None, None),) * 3 + (P("rep", "dp", None),) * 6,
        check_vma=False,
    )
```

```python
import functools

import jax
import jax.numpy as jnp
from jax import lax
from jax.experimental import pallas as pl
from jax.experimental.pallas import tpu as pltpu
from jax.sharding import PartitionSpec as P


BF, F32 = jnp.bfloat16, jnp.float32
ANY = pl.BlockSpec(memory_space=pl.ANY)
X, Y, CORE = 4, 2, 1
LANES = 640
ROWS = 16
RING = 6


class Weight:
    def __init__(self, w, cuts, split=None):
        self.block, self.cols, self.cuts, self.split = w.shape[1] // 8, w.shape[2], cuts, split
        self.gathered = split is None
        self.shape = 0 if self.cols == 1280 else 1
        assert sum(cuts) == self.block and (split is None or split in [sum(cuts[:i]) for i in range(len(cuts))])


def step_kernel(weights, *refs):
    n = len(weights)
    plan = [(i, sum(k.cuts[:j]), rows) for i, k in enumerate(weights) for j, rows in enumerate(k.cuts)]
    steps = len(plan)
    refs = list(refs)

    def take(count):
        out = refs[:count]
        del refs[:count]
        return out

    g, w, m, v = take(n), take(n), take(n), take(n)
    g_out = take(n)
    new = [take(1)[0] if k.gathered else take(8) for k in weights]
    late = take(2)
    from_core, from_x, from_y = take(n), take(n), take(n)
    in1, out1, in2, out2, in3, old_w, mv, g3, new3 = (take(2) for _ in range(9))
    core_send, core_recv, soon_send, soon_recv, load1, send1, load2, send2, recv_x, recv_y, load3, save3, own_send, own_recv, hop_send, hop_recv, twin_send, twin_recv, twin2_send, twin2_recv = refs

    me = lax.axis_index("dp")

    def to(mask):
        return dict(device_id={"dp": me ^ mask}, device_id_type=pl.DeviceIdType.MESH)

    def which(t):
        wt, first, size = plan[t]
        return wt, weights[wt].shape, first, size

    def rows(t, device):
        wt, _, first, size = which(t)
        return pl.ds(pl.multiple_of(device * weights[wt].block + first, 16), size)

    def mine(t):
        return pl.ds(plan[t][1], plan[t][2])

    def held(t, ref, *at):
        ref = ref[which(t)[1]]
        return ref.at[(t % ref.shape[0], *at, pl.ds(0, plan[t][2]))]

    def vector(t, units, body):
        wt, s, _, size = which(t)
        down, across = size // ROWS, weights[wt].cols // LANES

        @pl.loop(0, units * down * across)
        def _(i):
            u = i // (down * across)
            j = i % (down * across)
            r = pl.multiple_of((j // across) * ROWS, ROWS)
            c = pl.multiple_of((j % across) * LANES, 128)
            body(s, t % 2, u, (pl.ds(r, ROWS), pl.ds(c, LANES)))

    targets = (X ^ Y, X, Y, 0)

    def core_copies(t):
        for q in range(4):
            if t == 0 and q == 0:
                continue
            at = (1 if q == 1 else 0) if t == 0 and q in (1, 2) else slice(None)
            yield pltpu.make_async_remote_copy(
                g[plan[t][0]].at[at, rows(t, me ^ CORE ^ targets[q])],
                from_core[plan[t][0]].at[q, at, mine(t)],
                core_send.at[t % RING, q] if t else soon_send.at[4 + q],
                core_recv.at[t % RING, q] if t else soon_recv.at[4 + q],
                **to(CORE),
            )

    units1 = ((0, 0), (1, 0), (0, 1), (2, 1))

    def own1(t, u):
        q, layer = units1[u]
        return pltpu.make_async_copy(g[plan[t][0]].at[layer, rows(t, me ^ targets[q])], held(t, in1, u, 0), load1.at[u, 0])

    def twin1(t, u):
        q, layer = units1[u]
        return pltpu.make_async_copy(from_core[plan[t][0]].at[q, layer, mine(t)], held(t, in1, u, 1), load1.at[u, 1])

    def soon(u):
        q, layer = units1[u]
        return pltpu.make_async_remote_copy(
            g[plan[0][0]].at[layer, rows(0, me ^ CORE ^ targets[q])], held(0, in1, u, 1), soon_send.at[u], soon_recv.at[u], **to(CORE)
        )

    def merged(t):
        return 3 <= t < steps - 2

    def order1(t):
        return (0, 2) if merged(t) else (0, 2, 1, 3)

    def go1(t, u):
        mask, dst, sem = ((X, from_x, recv_x), (Y, from_y, recv_y))[u // 2]
        count = 2 if merged(t) else 1
        return pltpu.make_async_remote_copy(
            held(t, out1, pl.ds(u, count)), dst[plan[t][0]].at[pl.ds(u % 2, count), mine(t)], send1.at[t % 2, u], sem.at[t % RING, u % 2], **to(mask)
        )

    units2 = ((2, 0, from_x, Y, from_y, recv_y), (1, 1, from_y, X, from_x, recv_x))

    def loads2(t, u):
        wt = plan[t][0]
        q, layer, src = units2[u][:3]
        sources = (g[wt].at[layer, rows(t, me ^ targets[q])], from_core[wt].at[q, layer, mine(t)], src[wt].at[0, mine(t)])
        return [pltpu.make_async_copy(r, held(t, in2, u, i), load2.at[u, i]) for i, r in enumerate(sources)]

    def go2(t, u):
        mask, dst, sem = units2[u][3:]
        return pltpu.make_async_remote_copy(held(t, out2, u), dst[plan[t][0]].at[2, mine(t)], send2.at[t % 2, u], sem.at[t % RING, 2], **to(mask))

    def loads3(t, layer):
        wt = plan[t][0]
        straight, summed = (from_x, from_y) if layer == 0 else (from_y, from_x)
        moves = [
            (g[wt].at[layer, rows(t, me)], held(t, in3, layer, 0)),
            (from_core[wt].at[3, layer, mine(t)], held(t, in3, layer, 1)),
            (w[wt].at[layer, rows(t, me)], held(t, old_w, layer)),
            (m[wt].at[layer, mine(t)], held(t, mv, layer, 0)),
            (v[wt].at[layer, mine(t)], held(t, mv, layer, 1)),
            (straight[wt].at[1, mine(t)], held(t, in3, layer, 2)),
            (summed[wt].at[2, mine(t)], held(t, in3, layer, 3)),
        ]
        return [pltpu.make_async_copy(a, b, load3.at[layer, i]) for i, (a, b) in enumerate(moves)]

    def piece(t, layer):
        wt, _, first, _ = which(t)
        k = weights[wt]
        return (new[wt][2 + 2 * layer], first) if first < k.split else (new[wt][3 + 2 * layer], first - k.split)

    def saves3(t, layer):
        wt, _, _, size = which(t)
        places = [g_out[wt].at[layer, mine(t)]]
        if weights[wt].gathered:
            places.append(new[wt].at[layer, rows(t, me)])
        else:
            ref, at = piece(t, layer)
            places += [new[wt][layer].at[mine(t)], ref.at[pl.ds(at, size)]]
        return [
            pltpu.make_async_copy(held(t, g3 if i == 0 else new3, layer), place, save3.at[t % 2, layer, i]) for i, place in enumerate(places)
        ]

    masks = (X, Y, CORE)

    def layers(t):
        return (pl.ds(0, 2),) if merged(t) and gathered(t) else (0, 1)

    def number(layer):
        return layer if isinstance(layer, int) else 0

    def own_copy(t, layer, i):
        wt = plan[t][0]
        dst = new[wt].at[layer, rows(t, me)] if weights[wt].gathered else new[wt][6 + layer].at[mine(t)]
        k = number(layer)
        return pltpu.make_async_remote_copy(held(t, new3, layer), dst, own_send.at[t % 2, k, i], own_recv.at[t % RING, k, i], **to(masks[i]))

    def own_copies(t):
        if not gathered(t):
            return [own_copy(t, layer, 2) for layer in layers(t)]
        if merged(t):
            return [own_copy(t, layer, i) for layer in layers(t) for i in range(3)]
        return [own_copy(t, layer, i) for layer, i in ((0, 0), (1, 1), (1, 0), (0, 1), (0, 2), (1, 2))]

    def pass_copy(t, layer, source, target, send, recv, dst=None):
        place = new[plan[t][0]].at[layer, rows(t, me ^ source)]
        return pltpu.make_async_remote_copy(place, place if dst is None else dst, send, recv, **to(target))

    def hop(t, layer):
        source, target = ((X, Y), (Y, X))[layer]
        return pass_copy(t, layer, source, target, hop_send.at[t % RING, layer], hop_recv.at[t % RING, layer], late[layer] if t == steps - 1 else None)

    def twin(t, layer, i):
        k = number(layer)
        return pass_copy(t, layer, masks[i], CORE, twin_send.at[t % RING, k, i], twin_recv.at[t % RING, k, i])

    def twin2(t, layer):
        return pass_copy(t, layer, X ^ Y, CORE, twin2_send.at[t % RING, layer], twin2_recv.at[t % RING, layer])

    def real(t):
        return 0 <= t < steps

    def gathered(t):
        return real(t) and weights[plan[t][0]].gathered

    for u in range(4):
        own1(0, u).start()
    barrier = pltpu.get_barrier_semaphore()
    for mask in masks:
        pl.semaphore_signal(barrier, inc=1, **to(mask))
    pl.semaphore_wait(barrier, 3)

    def start_core(t):
        for c in core_copies(t):
            c.start()

    def prepare1(t):
        for c in core_copies(t):
            c.wait_recv()
        for u in range(4):
            twin1(t, u).start()

    for u in range(4):
        soon(u).start()
    start_core(0)
    start_core(1)
    for t in range(steps + 5):
        if real(t + 2):
            if t + 2 - RING >= 1:
                for c in core_copies(t + 2 - RING):
                    c.wait_send()
            start_core(t + 2)
        if real(t):
            for u in range(4):
                own1(t, u).wait()
                if t == 0:
                    soon(u).wait_recv()
                else:
                    twin1(t, u).wait()
            if t >= 2:
                for u in order1(t - 2):
                    go1(t - 2, u).wait_send()

            def sum1(s, slot, u, at):
                out1[s][slot, u, *at] = (in1[s][0, u, 0, *at].astype(F32) + in1[s][0, u, 1, *at].astype(F32)).astype(BF)

            vector(t, 4, sum1)
            for u in order1(t):
                go1(t, u).start()
        if real(t + 1):
            for u in range(4):
                own1(t + 1, u).start()
            prepare1(t + 1)
        a = t - 1
        if real(a):
            if a == 0:
                for c in core_copies(0):
                    c.wait_recv()
            for u in range(2):
                for c in loads2(a, u)[:2]:
                    c.start()
            for u in range(2):
                go1(a, 2 * u).wait_recv()
                loads2(a, u)[2].start()
            for u in range(2):
                for c in loads2(a, u):
                    c.wait()
                if a >= 2:
                    go2(a - 2, u).wait_send()

            def sum2(s, slot, u, at):
                out2[s][slot, u, *at] = (
                    in2[s][0, u, 0, *at].astype(F32) + in2[s][0, u, 1, *at].astype(F32) + in2[s][0, u, 2, *at].astype(F32)
                ).astype(BF)

            vector(a, 2, sum2)
            for u in range(2):
                go2(a, u).start()
        b = t - 2
        if real(b):
            for layer in range(2):
                for c in loads3(b, layer)[:5]:
                    c.start()
            for layer in range(2):
                if not merged(b):
                    go1(b, 1 + 2 * layer).wait_recv()
                go2(b, layer).wait_recv()
                for c in loads3(b, layer)[5:]:
                    c.start()
            for layer in range(2):
                for c in loads3(b, layer):
                    c.wait()
                if b >= 2:
                    for c in saves3(b - 2, layer):
                        c.wait()

            if b >= 2:
                for c in own_copies(b - 2):
                    c.wait_send()

            def update(s, slot, u, at):
                parts = [in3[s][0, u, i, *at].astype(F32) for i in range(4)]
                total = (((parts[0] + parts[1]) + parts[2]) + parts[3]).astype(BF)
                g3[s][slot, u, *at] = total
                total = total.astype(F32)
                new_m = 0.9 * mv[s][0, u, 0, *at] + 0.1 * total
                new_v = 0.95 * mv[s][0, u, 1, *at] + 0.05 * total * total
                weight = old_w[s][0, u, *at].astype(F32)
                new3[s][slot, u, *at] = (weight - 0.02 * (new_m * lax.rsqrt(new_v + 1e-8) + 0.1 * weight)).astype(BF)

            vector(b, 2, update)
            for c in own_copies(b):
                c.start()
            for layer in range(2):
                for c in saves3(b, layer):
                    c.start()
        c3 = t - 3
        if gathered(c3):
            if merged(c3):
                for i in range(2):
                    own_copy(c3, layers(c3)[0], i).wait_recv()
                for layer in range(2):
                    hop(c3, layer).start()
                for i in range(2):
                    twin(c3, layers(c3)[0], i).start()
            else:
                for layer in range(2):
                    own_copy(c3, layer, layer).wait_recv()
                    hop(c3, layer).start()
                    twin(c3, layer, layer).start()
                for layer in range(2):
                    own_copy(c3, layer, 1 - layer).wait_recv()
                    twin(c3, layer, 1 - layer).start()
        c4 = t - 4
        if gathered(c4):
            for layer in range(2):
                hop(c4, layer).wait_recv()
                if c4 < steps - 1:
                    twin2(c4, layer).start()

        if real(c4):
            for layer in layers(c4):
                own_copy(c4, layer, 2).wait_recv()
        c5 = t - 5
        if real(c5):
            if gathered(c5):
                for layer in layers(c5):
                    for i in range(2):
                        twin(c5, layer, i).wait()
                for layer in range(2):
                    hop(c5, layer).wait_send()
                    if c5 < steps - 1:
                        twin2(c5, layer).wait()

    for u in range(4):
        soon(u).wait_send()
    for t in (0, *range(max(1, steps - RING), steps)):
        for c in core_copies(t):
            c.wait_send()
    for t in range(steps - 2, steps):
        for u in order1(t):
            go1(t, u).wait_send()
        for u in range(2):
            go2(t, u).wait_send()
            for c in saves3(t, u):
                c.wait()
        for c in own_copies(t):
            c.wait_send()


def reduce_and_step(g, w, m, v, cuts, split):
    weights = [Weight(one, cut, split if i == 0 else None) for i, (one, cut) in enumerate(zip(w, cuts, strict=True))]
    n = len(w)
    pair = [max((max(k.cuts), k.cols) for k in weights if k.shape == s) for s in (0, 1)]

    def hbm(*lead):
        return [jax.ShapeDtypeStruct((*lead, k.block, k.cols), BF) for k in weights]

    def vmem(*lead, dtype=BF):
        return [pltpu.VMEM((*lead, *d), dtype) for d in pair]

    out_shape = hbm(2)
    for k in weights:
        sizes = (k.block, k.block, k.split, k.block - k.split, k.split, k.block - k.split, k.block, k.block) if k.split else ()
        out_shape += [jax.ShapeDtypeStruct((size, k.cols), BF) for size in sizes] or [jax.ShapeDtypeStruct((2, 8 * k.block, k.cols), BF)]
    out_shape += [jax.ShapeDtypeStruct((weights[-1].cuts[-1], weights[-1].cols), BF)] * 2
    out_shape += hbm(4, 2) + hbm(3) + hbm(3)
    dma = pltpu.SemaphoreType.DMA
    outs = pl.pallas_call(
        functools.partial(step_kernel, weights),
        out_shape=out_shape,
        in_specs=[ANY] * (4 * n),
        out_specs=[ANY] * len(out_shape),
        scratch_shapes=[
            *vmem(1, 4, 2),
            *vmem(2, 4),
            *vmem(1, 2, 3),
            *vmem(2, 2),
            *vmem(1, 2, 4),
            *vmem(1, 2),
            *vmem(1, 2, 2, dtype=F32),
            *vmem(2, 2),
            *vmem(2, 2),
            dma((RING, 4)),
            dma((RING, 4)),
            dma((8,)),
            dma((8,)),
            dma((4, 2)),
            dma((2, 4)),
            dma((2, 3)),
            dma((2, 2)),
            dma((RING, 3)),
            dma((RING, 3)),
            dma((2, 7)),
            dma((2, 2, 3)),
            dma((2, 2, 3)),
            dma((RING, 2, 3)),
            dma((RING, 2)),
            dma((RING, 2)),
            dma((RING, 2, 2)),
            dma((RING, 2, 2)),
            dma((RING, 2)),
            dma((RING, 2)),
        ],
        compiler_params=pltpu.CompilerParams(collective_id=0, has_side_effects=True, vmem_limit_bytes=60 << 20),
        cost_estimate=pl.CostEstimate(flops=10**9, bytes_accessed=4 * 10**8, transcendentals=10**7),
        name="reduce_and_step",
    )(*g, *w, *m, *v)
    return outs[:n], outs[n : n + 8], outs[n + 8 : 2 * n + 7], outs[2 * n + 7 : 2 * n + 9]


def cost(bytes_accessed, flops):
    return pl.CostEstimate(flops=flops, bytes_accessed=bytes_accessed, transcendentals=0)


def copied(x):
    layers, rows, cols = x.shape
    part, slots = rows // 8, 8
    pieces = [(layer, i) for layer in range(layers) for i in range(8)]

    def body(src, dst, held, sem_in, sem_out):
        def get(j):
            layer, i = pieces[j]
            return pltpu.make_async_copy(src.at[layer, pl.ds(i * part, part)], held.at[j % slots], sem_in.at[j % slots])

        def put(j):
            layer, i = pieces[j]
            return pltpu.make_async_copy(held.at[j % slots], dst.at[layer, pl.ds(i * part, part)], sem_out.at[j % slots])

        lag = slots // 2
        for j in range(len(pieces) + lag):
            if j < len(pieces):
                if j >= slots:
                    put(j - slots).wait()
                get(j).start()
            if j >= lag:
                get(j - lag).wait()
                put(j - lag).start()
        for j in range(len(pieces) - slots, len(pieces)):
            put(j).wait()

    return pl.pallas_call(
        body,
        out_shape=jax.ShapeDtypeStruct(x.shape, x.dtype),
        in_specs=[ANY],
        out_specs=ANY,
        scratch_shapes=[pltpu.VMEM((slots, part, cols), x.dtype), pltpu.SemaphoreType.DMA((slots,)), pltpu.SemaphoreType.DMA((slots,))],
        cost_estimate=cost(4 * x.size, 10**8),
        compiler_params=pltpu.CompilerParams(vmem_limit_bytes=16 << 20),
        name="copied",
    )(x)


def placed(pieces, out, block, near=True):
    n, cols = len(pieces), pieces[0][0].shape[-1]

    def body(*refs):
        src, (dst, *held, sem) = refs[:n], refs[n if out is None else n + 1 :]
        me = lax.axis_index("dp")
        if not near:
            gets = [pltpu.make_async_copy(a, b, sem.at[n + i]) for i, (a, b) in enumerate(zip(src, held, strict=True))]
            for c in gets:
                c.start()
            src = held
        puts = []
        for i, (one, layer, mask, first) in enumerate(pieces):
            to = pl.ds(pl.multiple_of((me ^ mask) * block + first, 16), one.shape[0])
            puts.append(pltpu.make_async_copy(src[i], dst.at[layer, to], sem.at[i]))
            if not near:
                gets[i].wait()
            puts[i].start()
        for c in puts:
            c.wait()

    args = [one[0] for one in pieces] + ([] if out is None else [out])
    scratch = [] if near else [pltpu.VMEM(one[0].shape, BF) for one in pieces]
    return pl.pallas_call(
        body,
        out_shape=jax.ShapeDtypeStruct((2, block * 8, cols), BF),
        in_specs=[pl.BlockSpec(memory_space=pltpu.VMEM) if near else ANY] * n + [ANY] * (len(args) - n),
        out_specs=ANY,
        input_output_aliases={} if out is None else {n: 0},
        scratch_shapes=[*scratch, pltpu.SemaphoreType.DMA((2 * n,))],
        cost_estimate=cost(4 * sum(one[0].size for one in pieces), 10**7),
        compiler_params=pltpu.CompilerParams(vmem_limit_bytes=8 << 20),
        name="placed",
    )(*args)


def moved(x, mask):
    return lax.ppermute(x, "dp", [(i, i ^ mask) for i in range(8)])


def moments(m, v, g):
    g = g.astype(F32)
    return 0.9 * m + 0.1 * g, 0.95 * v + 0.05 * g * g


CUTS = ((32, 64, 96, 112, 128, 128), (80, 80), (80, 48, 32))
SPLIT = 432


def solution(mesh):
    def inner(*arrays):
        terms, weights, m, v = (arrays[i : i + 3] for i in (0, 3, 6, 9))
        order = (2, 0, 1)
        sums, mine, (gate, up), late = reduce_and_step(
            [terms[i][0] for i in order], [weights[i] for i in order], [m[i] for i in order], [v[i] for i in order], CUTS, SPLIT
        )
        sums = [sums[order.index(i)] for i in range(3)]
        A, B, A0, A1, B0, B1, cA, cB = mine
        rows = A.shape[0]
        xA0, yB0, xA1, yB1 = moved(A0, X), moved(B0, Y), moved(A1, X), moved(B1, Y)
        xB, yA = moved(B, X), moved(A, Y)
        dA0, dB0, dA1, dB1 = moved(xA0, Y), moved(yB0, X), moved(xA1, Y), moved(yB1, X)
        gate = copied(gate)
        up = copied(up)

        def place(i, whole, *pieces, block=rows):
            return placed(pieces, whole, block, near=i > 0)

        def twins(*pieces):
            return [(moved(x, CORE), layer, mask + CORE, first) for x, layer, mask, first in pieces]

        near = [(xA0, 0, X, 0), (yB0, 1, Y, 0), (xA1, 0, X, SPLIT), (yB1, 1, Y, SPLIT), (xB, 1, X, 0), (yA, 0, Y, 0)]
        far0, far1 = [(dA0, 0, X + Y, 0), (dB0, 1, X + Y, 0)], [(dA1, 0, X + Y, SPLIT), (dB1, 1, X + Y, SPLIT)]
        block = up.shape[1] // 8
        far = [(x, layer, X + Y, block - CUTS[2][-1]) for layer, x in enumerate(late)]
        up = place(7, up, *far, *twins(*far), block=block)
        down = place(0, None, (A, 0, 0, 0), (B, 1, 0, 0), (cA, 0, CORE, 0), (cB, 1, CORE, 0))
        down = place(1, down, *near)
        down = place(2, down, *twins(*near))
        down = place(3, down, *far0)
        down = place(4, down, *twins(*far0))
        down = place(5, down, *far1)
        last = [(moved(x, CORE), layer, mask + CORE, first) for x, layer, mask, first in far1]
        down = place(6, down, *last)
        after = []
        for i in range(3):
            after.append(moments(m[i], v[i], sums[i]))
        return (gate, up, down, *(one[0] for one in after), *(one[1] for one in after))

    all_of, cut = P(None, None, None), P(None, "dp", None)
    return jax.shard_map(
        inner,
        mesh=mesh,
        in_specs=(P(("rep", "dp"), None, None, None),) * 3 + (all_of,) * 3 + (cut,) * 6,
        out_specs=(P("rep", None, None),) * 3 + (P("rep", "dp", None),) * 6,
        check_vma=False,
    )
```

```python
import functools

import jax
import jax.numpy as jnp
from jax import lax
from jax.experimental import pallas as pl
from jax.experimental.pallas import tpu as pltpu
from jax.sharding import PartitionSpec as P


BF, F32 = jnp.bfloat16, jnp.float32
ANY = pl.BlockSpec(memory_space=pl.ANY)
X, Y, CORE = 4, 2, 1
LANES = 640
ROWS = 16
RING = 5


class Weight:
    def __init__(self, w, cuts, split=None):
        self.block, self.cols, self.cuts, self.split = w.shape[1] // 8, w.shape[2], cuts, split
        self.gathered = split is None
        self.shape = 0 if self.cols == 1280 else 1
        assert sum(cuts) == self.block and (split is None or split in [sum(cuts[:i]) for i in range(len(cuts))])


def step_kernel(weights, *refs):
    n = len(weights)
    plan = [(i, sum(k.cuts[:j]), rows) for i, k in enumerate(weights) for j, rows in enumerate(k.cuts)]
    steps = len(plan)
    refs = list(refs)

    def take(count):
        out = refs[:count]
        del refs[:count]
        return out

    g, w, m, v = take(n), take(n), take(n), take(n)
    g_out = take(n)
    new = [take(1)[0] if k.gathered else take(8) for k in weights]
    late = take(2)
    from_core, from_x, from_y = take(n), take(n), take(n)
    in1, out1, in2, out2, in3, old_w, mv, g3, new3 = (take(2) for _ in range(9))
    core_send, core_recv, soon_send, soon_recv, load1, send1, load2, send2, recv_x, recv_y, load3, save3, own_send, own_recv, hop_send, hop_recv, twin_send, twin_recv, twin2_send, twin2_recv = refs

    me = lax.axis_index("dp")

    def to(mask):
        return dict(device_id={"dp": me ^ mask}, device_id_type=pl.DeviceIdType.MESH)

    def which(t):
        wt, first, size = plan[t]
        return wt, weights[wt].shape, first, size

    def rows(t, device):
        wt, _, first, size = which(t)
        return pl.ds(pl.multiple_of(device * weights[wt].block + first, 16), size)

    def mine(t):
        return pl.ds(plan[t][1], plan[t][2])

    def held(t, ref, *at):
        ref = ref[which(t)[1]]
        return ref.at[(t % ref.shape[0], *at, pl.ds(0, plan[t][2]))]

    def vector(t, units, body):
        wt, s, _, size = which(t)
        down, across = size // ROWS, weights[wt].cols // LANES

        @pl.loop(0, units * down * across)
        def _(i):
            u = i // (down * across)
            j = i % (down * across)
            r = pl.multiple_of((j // across) * ROWS, ROWS)
            c = pl.multiple_of((j % across) * LANES, 128)
            body(s, t % 2, u, (pl.ds(r, ROWS), pl.ds(c, LANES)))

    targets = (X ^ Y, X, Y, 0)

    def core_copies(t):
        for q in range(4):
            if t == 0 and q == 0:
                continue
            at = (1 if q == 1 else 0) if t == 0 and q in (1, 2) else slice(None)
            yield pltpu.make_async_remote_copy(
                g[plan[t][0]].at[at, rows(t, me ^ CORE ^ targets[q])],
                from_core[plan[t][0]].at[q, at, mine(t)],
                core_send.at[t % RING, q] if t else soon_send.at[4 + q],
                core_recv.at[t % RING, q] if t else soon_recv.at[4 + q],
                **to(CORE),
            )

    units1 = ((0, 0), (1, 0), (0, 1), (2, 1))

    def own1(t, u):
        q, layer = units1[u]
        return pltpu.make_async_copy(g[plan[t][0]].at[layer, rows(t, me ^ targets[q])], held(t, in1, u, 0), load1.at[u, 0])

    def twin1(t, u):
        q, layer = units1[u]
        return pltpu.make_async_copy(from_core[plan[t][0]].at[q, layer, mine(t)], held(t, in1, u, 1), load1.at[u, 1])

    def soon(u):
        q, layer = units1[u]
        return pltpu.make_async_remote_copy(
            g[plan[0][0]].at[layer, rows(0, me ^ CORE ^ targets[q])], held(0, in1, u, 1), soon_send.at[u], soon_recv.at[u], **to(CORE)
        )

    def merged(t):
        return 3 <= t < steps - 2

    def order1(t):
        return (0, 2) if merged(t) else (0, 2, 1, 3)

    def go1(t, u):
        mask, dst, sem = ((X, from_x, recv_x), (Y, from_y, recv_y))[u // 2]
        count = 2 if merged(t) else 1
        return pltpu.make_async_remote_copy(
            held(t, out1, pl.ds(u, count)), dst[plan[t][0]].at[pl.ds(u % 2, count), mine(t)], send1.at[t % 2, u], sem.at[t % RING, u % 2], **to(mask)
        )

    units2 = ((2, 0, from_x, Y, from_y, recv_y), (1, 1, from_y, X, from_x, recv_x))

    def loads2(t, u):
        wt = plan[t][0]
        q, layer, src = units2[u][:3]
        sources = (g[wt].at[layer, rows(t, me ^ targets[q])], from_core[wt].at[q, layer, mine(t)], src[wt].at[0, mine(t)])
        return [pltpu.make_async_copy(r, held(t, in2, u, i), load2.at[u, i]) for i, r in enumerate(sources)]

    def go2(t, u):
        mask, dst, sem = units2[u][3:]
        return pltpu.make_async_remote_copy(held(t, out2, u), dst[plan[t][0]].at[2, mine(t)], send2.at[t % 2, u], sem.at[t % RING, 2], **to(mask))

    def loads3(t, layer):
        wt = plan[t][0]
        straight, summed = (from_x, from_y) if layer == 0 else (from_y, from_x)
        moves = [
            (g[wt].at[layer, rows(t, me)], held(t, in3, layer, 0)),
            (from_core[wt].at[3, layer, mine(t)], held(t, in3, layer, 1)),
            (w[wt].at[layer, rows(t, me)], held(t, old_w, layer)),
            (m[wt].at[layer, mine(t)], held(t, mv, layer, 0)),
            (v[wt].at[layer, mine(t)], held(t, mv, layer, 1)),
            (straight[wt].at[1, mine(t)], held(t, in3, layer, 2)),
            (summed[wt].at[2, mine(t)], held(t, in3, layer, 3)),
        ]
        return [pltpu.make_async_copy(a, b, load3.at[layer, i]) for i, (a, b) in enumerate(moves)]

    def piece(t, layer):
        wt, _, first, _ = which(t)
        k = weights[wt]
        return (new[wt][2 + 2 * layer], first) if first < k.split else (new[wt][3 + 2 * layer], first - k.split)

    def saves3(t, layer):
        wt, _, _, size = which(t)
        places = [g_out[wt].at[layer, mine(t)]]
        if weights[wt].gathered:
            places.append(new[wt].at[layer, rows(t, me)])
        else:
            ref, at = piece(t, layer)
            places += [new[wt][layer].at[mine(t)], ref.at[pl.ds(at, size)]]
        return [
            pltpu.make_async_copy(held(t, g3 if i == 0 else new3, layer), place, save3.at[t % 2, layer, i]) for i, place in enumerate(places)
        ]

    masks = (X, Y, CORE)

    def layers(t):
        return (pl.ds(0, 2),) if merged(t) and gathered(t) else (0, 1)

    def number(layer):
        return layer if isinstance(layer, int) else 0

    def own_copy(t, layer, i):
        wt = plan[t][0]
        dst = new[wt].at[layer, rows(t, me)] if weights[wt].gathered else new[wt][6 + layer].at[mine(t)]
        k = number(layer)
        return pltpu.make_async_remote_copy(held(t, new3, layer), dst, own_send.at[t % 2, k, i], own_recv.at[t % (RING + 1), k, i], **to(masks[i]))

    def own_copies(t):
        if not gathered(t):
            return [own_copy(t, layer, 2) for layer in layers(t)]
        if merged(t):
            return [own_copy(t, layer, i) for layer in layers(t) for i in range(3)]
        return [own_copy(t, layer, i) for layer, i in ((0, 0), (1, 1), (1, 0), (0, 1), (0, 2), (1, 2))]

    def pass_copy(t, layer, source, target, send, recv, dst=None):
        place = new[plan[t][0]].at[layer, rows(t, me ^ source)]
        return pltpu.make_async_remote_copy(place, place if dst is None else dst, send, recv, **to(target))

    def hop(t, layer):
        source, target = ((X, Y), (Y, X))[layer]
        return pass_copy(t, layer, source, target, hop_send.at[t % RING, layer], hop_recv.at[t % RING, layer], late[layer] if t == steps - 1 else None)

    def twin(t, i):
        return pass_copy(t, pl.ds(0, 2), masks[i], CORE, twin_send.at[t % RING, i], twin_recv.at[t % RING, i])

    def twin2(t):
        return pass_copy(t, pl.ds(0, 2), X ^ Y, CORE, twin2_send.at[t % RING], twin2_recv.at[t % RING])

    def real(t):
        return 0 <= t < steps

    def gathered(t):
        return real(t) and weights[plan[t][0]].gathered

    for u in range(4):
        own1(0, u).start()
    barrier = pltpu.get_barrier_semaphore()
    for mask in masks:
        pl.semaphore_signal(barrier, inc=1, **to(mask))
    pl.semaphore_wait(barrier, 3)

    def start_core(t):
        for c in core_copies(t):
            c.start()

    def prepare1(t):
        for c in core_copies(t):
            c.wait_recv()
        for u in range(4):
            twin1(t, u).start()

    for u in range(4):
        soon(u).start()
    start_core(0)
    start_core(1)
    for t in range(steps + 5):
        if real(t + 2):
            if t + 2 - RING >= 1:
                for c in core_copies(t + 2 - RING):
                    c.wait_send()
            start_core(t + 2)
        if real(t):
            for u in range(4):
                own1(t, u).wait()
                if t == 0:
                    soon(u).wait_recv()
                else:
                    twin1(t, u).wait()
            if t >= 2:
                for u in order1(t - 2):
                    go1(t - 2, u).wait_send()

            def sum1(s, slot, u, at):
                out1[s][slot, u, *at] = (in1[s][0, u, 0, *at].astype(F32) + in1[s][0, u, 1, *at].astype(F32)).astype(BF)

            vector(t, 4, sum1)
            for u in order1(t):
                go1(t, u).start()
        if real(t + 1):
            for u in range(4):
                own1(t + 1, u).start()
            prepare1(t + 1)
        a = t - 1
        if real(a):
            if a == 0:
                for c in core_copies(0):
                    c.wait_recv()
            for u in range(2):
                for c in loads2(a, u)[:2]:
                    c.start()
            for u in range(2):
                go1(a, 2 * u).wait_recv()
                loads2(a, u)[2].start()
            for u in range(2):
                for c in loads2(a, u):
                    c.wait()
                if a >= 2:
                    go2(a - 2, u).wait_send()

            def sum2(s, slot, u, at):
                out2[s][slot, u, *at] = (
                    in2[s][0, u, 0, *at].astype(F32) + in2[s][0, u, 1, *at].astype(F32) + in2[s][0, u, 2, *at].astype(F32)
                ).astype(BF)

            vector(a, 2, sum2)
            for u in range(2):
                go2(a, u).start()
        b = t - 2
        if real(b):
            for layer in range(2):
                for c in loads3(b, layer)[:5]:
                    c.start()
            for layer in range(2):
                if not merged(b):
                    go1(b, 1 + 2 * layer).wait_recv()
                go2(b, layer).wait_recv()
                for c in loads3(b, layer)[5:]:
                    c.start()
            for layer in range(2):
                for c in loads3(b, layer):
                    c.wait()
                if b >= 2:
                    for c in saves3(b - 2, layer):
                        c.wait()

            if b >= 2:
                for c in own_copies(b - 2):
                    c.wait_send()

            def update(s, slot, u, at):
                parts = [in3[s][0, u, i, *at].astype(F32) for i in range(4)]
                total = (((parts[0] + parts[1]) + parts[2]) + parts[3]).astype(BF)
                g3[s][slot, u, *at] = total
                total = total.astype(F32)
                new_m = 0.9 * mv[s][0, u, 0, *at] + 0.1 * total
                new_v = 0.95 * mv[s][0, u, 1, *at] + 0.05 * total * total
                weight = old_w[s][0, u, *at].astype(F32)
                new3[s][slot, u, *at] = (weight - 0.02 * (new_m * lax.rsqrt(new_v + 1e-8) + 0.1 * weight)).astype(BF)

            vector(b, 2, update)
            for c in own_copies(b):
                c.start()
            for layer in range(2):
                for c in saves3(b, layer):
                    c.start()
        c3 = t - 3
        if gathered(c3):
            if merged(c3):
                for i in range(2):
                    own_copy(c3, layers(c3)[0], i).wait_recv()
                for layer in range(2):
                    hop(c3, layer).start()
            else:
                for layer in range(2):
                    own_copy(c3, layer, layer).wait_recv()
                    hop(c3, layer).start()
                for layer in range(2):
                    own_copy(c3, layer, 1 - layer).wait_recv()
            for i in range(2):
                twin(c3, i).start()
        c4 = t - 4
        if gathered(c4):
            for layer in range(2):
                hop(c4, layer).wait_recv()
            if c4 < steps - 1:
                twin2(c4).start()

        if real(c4):
            for layer in layers(c4):
                own_copy(c4, layer, 2).wait_recv()
        c5 = t - 5
        if real(c5):
            if gathered(c5):
                for i in range(2):
                    twin(c5, i).wait()
                for layer in range(2):
                    hop(c5, layer).wait_send()
                if c5 < steps - 1:
                    twin2(c5).wait()

    for u in range(4):
        soon(u).wait_send()
    for t in (0, *range(max(1, steps - RING), steps)):
        for c in core_copies(t):
            c.wait_send()
    for t in range(steps - 2, steps):
        for u in order1(t):
            go1(t, u).wait_send()
        for u in range(2):
            go2(t, u).wait_send()
            for c in saves3(t, u):
                c.wait()
        for c in own_copies(t):
            c.wait_send()


def reduce_and_step(g, w, m, v, cuts, split):
    weights = [Weight(one, cut, split if i == 0 else None) for i, (one, cut) in enumerate(zip(w, cuts, strict=True))]
    n = len(w)
    pair = [max((max(k.cuts), k.cols) for k in weights if k.shape == s) for s in (0, 1)]

    def hbm(*lead):
        return [jax.ShapeDtypeStruct((*lead, k.block, k.cols), BF) for k in weights]

    def vmem(*lead, dtype=BF):
        return [pltpu.VMEM((*lead, *d), dtype) for d in pair]

    out_shape = hbm(2)
    for k in weights:
        sizes = (k.block, k.block, k.split, k.block - k.split, k.split, k.block - k.split, k.block, k.block) if k.split else ()
        out_shape += [jax.ShapeDtypeStruct((size, k.cols), BF) for size in sizes] or [jax.ShapeDtypeStruct((2, 8 * k.block, k.cols), BF)]
    out_shape += [jax.ShapeDtypeStruct((weights[-1].cuts[-1], weights[-1].cols), BF)] * 2
    out_shape += hbm(4, 2) + hbm(3) + hbm(3)
    dma = pltpu.SemaphoreType.DMA
    outs = pl.pallas_call(
        functools.partial(step_kernel, weights),
        out_shape=out_shape,
        in_specs=[ANY] * (4 * n),
        out_specs=[ANY] * len(out_shape),
        scratch_shapes=[
            *vmem(1, 4, 2),
            *vmem(2, 4),
            *vmem(1, 2, 3),
            *vmem(2, 2),
            *vmem(1, 2, 4),
            *vmem(1, 2),
            *vmem(1, 2, 2, dtype=F32),
            *vmem(2, 2),
            *vmem(2, 2),
            dma((RING, 4)),
            dma((RING, 4)),
            dma((8,)),
            dma((8,)),
            dma((4, 2)),
            dma((2, 4)),
            dma((2, 3)),
            dma((2, 2)),
            dma((RING, 3)),
            dma((RING, 3)),
            dma((2, 7)),
            dma((2, 2, 3)),
            dma((2, 2, 3)),
            dma((RING + 1, 2, 3)),
            dma((RING, 2)),
            dma((RING, 2)),
            dma((RING, 2)),
            dma((RING, 2)),
            dma((RING,)),
            dma((RING,)),
        ],
        compiler_params=pltpu.CompilerParams(collective_id=0, has_side_effects=True, vmem_limit_bytes=60 << 20),
        cost_estimate=pl.CostEstimate(flops=10**9, bytes_accessed=4 * 10**8, transcendentals=10**7),
        name="reduce_and_step",
    )(*g, *w, *m, *v)
    return outs[:n], outs[n : n + 8], outs[n + 8 : 2 * n + 7], outs[2 * n + 7 : 2 * n + 9]


def cost(bytes_accessed, flops):
    return pl.CostEstimate(flops=flops, bytes_accessed=bytes_accessed, transcendentals=0)


def copied(x):
    layers, rows, cols = x.shape
    part, slots = rows // 8, 8
    pieces = [(layer, i) for layer in range(layers) for i in range(8)]

    def body(src, dst, held, sem_in, sem_out):
        def get(j):
            layer, i = pieces[j]
            return pltpu.make_async_copy(src.at[layer, pl.ds(i * part, part)], held.at[j % slots], sem_in.at[j % slots])

        def put(j):
            layer, i = pieces[j]
            return pltpu.make_async_copy(held.at[j % slots], dst.at[layer, pl.ds(i * part, part)], sem_out.at[j % slots])

        lag = slots // 2
        for j in range(len(pieces) + lag):
            if j < len(pieces):
                if j >= slots:
                    put(j - slots).wait()
                get(j).start()
            if j >= lag:
                get(j - lag).wait()
                put(j - lag).start()
        for j in range(len(pieces) - slots, len(pieces)):
            put(j).wait()

    return pl.pallas_call(
        body,
        out_shape=jax.ShapeDtypeStruct(x.shape, x.dtype),
        in_specs=[ANY],
        out_specs=ANY,
        scratch_shapes=[pltpu.VMEM((slots, part, cols), x.dtype), pltpu.SemaphoreType.DMA((slots,)), pltpu.SemaphoreType.DMA((slots,))],
        cost_estimate=cost(4 * x.size, 10**8),
        compiler_params=pltpu.CompilerParams(vmem_limit_bytes=16 << 20),
        name="copied",
    )(x)


def placed(pieces, out, block, near=True):
    n, cols = len(pieces), pieces[0][0].shape[-1]

    def body(*refs):
        src, (dst, *held, sem) = refs[:n], refs[n if out is None else n + 1 :]
        me = lax.axis_index("dp")
        if not near:
            gets = [pltpu.make_async_copy(a, b, sem.at[n + i]) for i, (a, b) in enumerate(zip(src, held, strict=True))]
            for c in gets:
                c.start()
            src = held
        puts = []
        for i, (one, layer, mask, first) in enumerate(pieces):
            to = pl.ds(pl.multiple_of((me ^ mask) * block + first, 16), one.shape[0])
            puts.append(pltpu.make_async_copy(src[i], dst.at[layer, to], sem.at[i]))
            if not near:
                gets[i].wait()
            puts[i].start()
        for c in puts:
            c.wait()

    args = [one[0] for one in pieces] + ([] if out is None else [out])
    scratch = [] if near else [pltpu.VMEM(one[0].shape, BF) for one in pieces]
    return pl.pallas_call(
        body,
        out_shape=jax.ShapeDtypeStruct((2, block * 8, cols), BF),
        in_specs=[pl.BlockSpec(memory_space=pltpu.VMEM) if near else ANY] * n + [ANY] * (len(args) - n),
        out_specs=ANY,
        input_output_aliases={} if out is None else {n: 0},
        scratch_shapes=[*scratch, pltpu.SemaphoreType.DMA((2 * n,))],
        cost_estimate=cost(4 * sum(one[0].size for one in pieces), 10**7),
        compiler_params=pltpu.CompilerParams(vmem_limit_bytes=8 << 20),
        name="placed",
    )(*args)


def moved(x, mask):
    return lax.ppermute(x, "dp", [(i, i ^ mask) for i in range(8)])


def moments(m, v, g):
    g = g.astype(F32)
    return 0.9 * m + 0.1 * g, 0.95 * v + 0.05 * g * g


CUTS = ((32, 64, 96, 112, 128, 128), (80, 80), (80, 48, 32))
SPLIT = 432


def solution(mesh):
    def inner(*arrays):
        terms, weights, m, v = (arrays[i : i + 3] for i in (0, 3, 6, 9))
        order = (2, 0, 1)
        sums, mine, (gate, up), late = reduce_and_step(
            [terms[i][0] for i in order], [weights[i] for i in order], [m[i] for i in order], [v[i] for i in order], CUTS, SPLIT
        )
        sums = [sums[order.index(i)] for i in range(3)]
        A, B, A0, A1, B0, B1, cA, cB = mine
        rows = A.shape[0]
        xA0, yB0, xA1, yB1 = moved(A0, X), moved(B0, Y), moved(A1, X), moved(B1, Y)
        xB, yA = moved(B, X), moved(A, Y)
        dA0, dB0, dA1, dB1 = moved(xA0, Y), moved(yB0, X), moved(xA1, Y), moved(yB1, X)
        gate = copied(gate)
        up = copied(up)

        def place(i, whole, *pieces, block=rows):
            return placed(pieces, whole, block, near=i > 0)

        def twins(*pieces):
            return [(moved(x, CORE), layer, mask + CORE, first) for x, layer, mask, first in pieces]

        near = [(xA0, 0, X, 0), (yB0, 1, Y, 0), (xA1, 0, X, SPLIT), (yB1, 1, Y, SPLIT), (xB, 1, X, 0), (yA, 0, Y, 0)]
        far0, far1 = [(dA0, 0, X + Y, 0), (dB0, 1, X + Y, 0)], [(dA1, 0, X + Y, SPLIT), (dB1, 1, X + Y, SPLIT)]
        block = up.shape[1] // 8
        far = [(x, layer, X + Y, block - CUTS[2][-1]) for layer, x in enumerate(late)]
        up = place(7, up, *far, *twins(*far), block=block)
        down = place(0, None, (A, 0, 0, 0), (B, 1, 0, 0), (cA, 0, CORE, 0), (cB, 1, CORE, 0))
        down = place(1, down, *near)
        down = place(2, down, *twins(*near))
        down = place(3, down, *far0)
        down = place(4, down, *twins(*far0))
        down = place(5, down, *far1)
        last = [(moved(x, CORE), layer, mask + CORE, first) for x, layer, mask, first in far1]
        down = place(6, down, *last)
        after = []
        for i in range(3):
            after.append(moments(m[i], v[i], sums[i]))
        return (gate, up, down, *(one[0] for one in after), *(one[1] for one in after))

    all_of, cut = P(None, None, None), P(None, "dp", None)
    return jax.shard_map(
        inner,
        mesh=mesh,
        in_specs=(P(("rep", "dp"), None, None, None),) * 3 + (all_of,) * 3 + (cut,) * 6,
        out_specs=(P("rep", None, None),) * 3 + (P("rep", "dp", None),) * 6,
        check_vma=False,
    )
```
